128 devices in a mesh: batch: 1, col: 16 (over z, y), row: 8 (over x, core).
Axes of the slice: x: 4, y: 4, z: 4, core: 2. Of those that a mesh axis runs over, the one named last changes fastest.
Arguments:
- d_inv: bfloat16 [64, 1024, 1024], P(('batch', 'row'))
- l_blk: bfloat16 [64, 1024, 1024], P(('batch', 'row'))
- u_blk: bfloat16 [64, 1024, 1024], P(('batch', 'row'))
- rhs_blk: float32 [64, 1024, 1536], P(('batch', 'row'), None, 'col')
- x_init: float32 [64, 1024, 1536], P(('batch', 'row'), None, 'col')
Outputs:
- output: float32 [64, 1024, 1536], P(('batch', 'row'), None, 'col')
All inputs are finite; a program needn't handle non-finite values.
Results may differ from the reference program's by a relative error of at most 0.0123155.
Values are sent between devices in bfloat16 or wider.
A program may use at most 1 GiB of HBM per device.

```python
import jax
import jax.numpy as jnp
from jax import lax

BLOCK_ROWS = 64
BLOCK_SIZE = 1024
RHS_COLS = 1536
SWEEPS = 4


def setup_inputs(seed: int = 0, part: int = 0) -> dict:
    base_key = jax.random.fold_in(jax.random.key(seed), part)
    k_d, k_l, k_u, k_f, k_x = jax.random.split(base_key, 5)
    fan_scale = BLOCK_SIZE ** -0.5
    mat_shape = (BLOCK_ROWS, BLOCK_SIZE, BLOCK_SIZE)
    vec_shape = (BLOCK_ROWS, BLOCK_SIZE, RHS_COLS)
    ident_mat = jnp.eye(BLOCK_SIZE, dtype=jnp.float32)
    row_ids = jnp.arange(BLOCK_ROWS)
    l_mask = (row_ids > 0).astype(jnp.float32)[:, None, None]
    u_mask = (row_ids < BLOCK_ROWS - 1).astype(jnp.float32)[:, None, None]
    d_inv = ident_mat + 0.3 * fan_scale * jax.random.normal(k_d, mat_shape, jnp.float32)
    l_blk = 0.6 * fan_scale * jax.random.normal(k_l, mat_shape, jnp.float32) * l_mask
    u_blk = 0.45 * fan_scale * jax.random.normal(k_u, mat_shape, jnp.float32) * u_mask
    rhs_blk = jax.random.normal(k_f, vec_shape, jnp.float32)
    x_init = jax.random.normal(k_x, vec_shape, jnp.float32)
    return {"d_inv": d_inv.astype(jnp.bfloat16), "l_blk": l_blk.astype(jnp.bfloat16), "u_blk": u_blk.astype(jnp.bfloat16), "rhs_blk": rhs_blk, "x_init": x_init}


def reference(d_inv, l_blk, u_blk, rhs_blk, x_init):
    zero_blk = jnp.zeros((BLOCK_SIZE, RHS_COLS), jnp.float32)

    def row_step(x_left, row_in):
        d_i, l_i, u_i, f_i, x_right = row_in
        t_i = (f_i
               - jnp.dot(l_i, x_left.astype(jnp.bfloat16), preferred_element_type=jnp.float32)
               - jnp.dot(u_i, x_right.astype(jnp.bfloat16), preferred_element_type=jnp.float32))
        x_i = jnp.dot(d_i, t_i.astype(jnp.bfloat16), preferred_element_type=jnp.float32)
        return x_i, x_i

    def one_sweep(x_old, unused):
        x_right = jnp.concatenate([x_old[1:], zero_blk[None]], axis=0)
        _, x_new = lax.scan(row_step, zero_blk, (d_inv, l_blk, u_blk, rhs_blk, x_right))
        return x_new, None

    x_final, _ = lax.scan(one_sweep, x_init, None, length=SWEEPS)
    return x_final
```

```python
import functools

import jax
import jax.numpy as jnp
from jax import lax
from jax.experimental import pallas as pl
from jax.experimental.pallas import tpu as pltpu
from jax.sharding import PartitionSpec as P

SWEEPS = 4
TILE = 256
MESH = pl.DeviceIdType.MESH
F32, BF16 = jnp.float32, jnp.bfloat16


def dot_nn(x, mat):
    return jnp.dot(x, mat, preferred_element_type=F32)


def dot_nt(x, mat):
    return lax.dot_general(x, mat, (((1,), (1,)), ((), ())), preferred_element_type=F32)


def kernel(chain_len, rows, d_hbm, l_hbm, u_hbm, f_hbm, x_hbm, out_hbm,
           d_v, l_v, u_v, f_t, g_t, xs, f_raw, x_raw, x_f32, out_st,
           d_sem, l_sem, u_sem, f_sem, x_sem, out_sem,
           fs_sem, fr_sem, bs_sem, br_sem):
    p = lax.axis_index("row")
    size = d_v.shape[1]
    tiles = size // TILE
    has_left, has_right = p > 0, p < chain_len - 1
    from_left, from_right = rows, rows + SWEEPS

    def mat_copies(i):
        return (pltpu.make_async_copy(u_hbm.at[i], u_v.at[i], u_sem.at[i]),
                pltpu.make_async_copy(l_hbm.at[i], l_v.at[i], l_sem.at[i]),
                pltpu.make_async_copy(d_hbm.at[i], d_v.at[i], d_sem.at[i]))

    def f_copy(i, slot):
        return pltpu.make_async_copy(f_hbm.at[i], f_raw.at[slot], f_sem.at[slot])

    def x_copy(i, slot):
        return pltpu.make_async_copy(x_hbm.at[i], x_raw.at[slot], x_sem.at[slot])

    def send_right(k):
        return pltpu.make_async_remote_copy(
            src_ref=xs.at[rows - 1], dst_ref=xs.at[from_left + k], send_sem=fs_sem.at[k], recv_sem=fr_sem.at[k],
            device_id={"row": p + 1}, device_id_type=MESH)

    def send_left(k):
        return pltpu.make_async_remote_copy(
            src_ref=xs.at[0], dst_ref=xs.at[from_right + k], send_sem=bs_sem.at[k], recv_sem=br_sem.at[k],
            device_id={"row": p - 1}, device_id_type=MESH)

    x_copy(0, 0).start()
    x_copy(1, 1).start()
    f_copy(0, 0).start()
    f_copy(1, 1).start()
    for i in range(2):
        for c in mat_copies(i):
            c.start()

    barrier = pltpu.get_barrier_semaphore()

    @pl.when(has_left)
    def _():
        pl.semaphore_signal(barrier, inc=1, device_id={"row": p - 1}, device_id_type=MESH)

    @pl.when(has_right)
    def _():
        pl.semaphore_signal(barrier, inc=1, device_id={"row": p + 1}, device_id_type=MESH)

    pl.semaphore_wait(barrier, has_left.astype(jnp.int32) + has_right.astype(jnp.int32))

    zero = jnp.zeros(xs.shape[1:], BF16)

    @pl.when(jnp.logical_not(has_left))
    def _():
        for k in range(SWEEPS):
            xs[from_left + k] = zero

    @pl.when(jnp.logical_not(has_right))
    def _():
        for k in range(SWEEPS):
            xs[from_right + k] = zero

    def load_x(i, slot):
        x_copy(i, slot).wait()
        xs[i] = x_raw[slot].T.astype(BF16)

    def transpose_in_place(ref, i):
        def at(a, b):
            return ref.at[i, a * TILE:(a + 1) * TILE, b * TILE:(b + 1) * TILE]
        for a in range(tiles):
            at(a, a)[...] = at(a, a)[...].T
            for b in range(a + 1, tiles):
                upper, lower = at(a, b)[...].T, at(b, a)[...].T
                at(a, b)[...] = lower
                at(b, a)[...] = upper

    load_x(0, 0)
    x_copy(2, 0).start()

    @pl.when(has_left)
    def _():
        send_left(0).start()

    def load_row(i, last=False):
        slot = lax.rem(i, 2)
        if not last:
            @pl.when(i + 2 < rows)
            def _():
                for c in mat_copies(i + 2):
                    c.start()
            load_x(i + 1, 1 - slot)

            @pl.when(i + 3 < rows)
            def _():
                x_copy(i + 3, 1 - slot).start()
        f_copy(i, slot).wait()
        f_t[i] = f_raw[slot].T

        @pl.when(i + 2 < rows)
        def _():
            f_copy(i + 2, slot).start()
        u_c, l_c, d_c = mat_copies(i)
        l_c.wait()
        transpose_in_place(l_v, i)
        d_c.wait()
        transpose_in_place(d_v, i)
        u_c.wait()
        if not last:
            g_t[i] = f_t[i] - dot_nt(xs[i + 1], u_v[i])

    @pl.loop(0, rows - 1)
    def _(i):
        load_row(i)
    load_row(rows - 1, last=True)

    def row(i, left, final):
        t = g_t[i] - dot_nn(xs[left], l_v[i])
        x = dot_nn(t.astype(BF16), d_v[i])
        xs[i] = x.astype(BF16)
        if final:
            st = lax.rem(i, 2)

            @pl.when(i >= 2)
            def _():
                pltpu.make_async_copy(out_st.at[st], out_hbm.at[i - 2], out_sem.at[st]).wait()
            out_st[st] = x.T
            pltpu.make_async_copy(out_st.at[st], out_hbm.at[i], out_sem.at[st]).start()

    def sweep(k, final):
        @pl.when(has_left)
        def _():
            send_left(k).wait_send()
            fwd = pltpu.make_async_remote_copy(
                src_ref=xs.at[rows - 1], dst_ref=xs.at[from_left + k], send_sem=fs_sem.at[k], recv_sem=fr_sem.at[k],
                device_id={"row": p - 1}, device_id_type=MESH)
            fwd.wait_recv()

        @pl.when(jnp.logical_and(has_right, k > 0))
        def _():
            send_right(k - 1).wait_send()

        row(0, from_left + k, final)
        if not final:
            @pl.when(has_left)
            def _():
                send_left(k + 1).start()

        @pl.loop(1, rows - 1)
        def _(i):
            row(i, i - 1, final)

        @pl.when(has_right)
        def _():
            bwd = pltpu.make_async_remote_copy(
                src_ref=xs.at[0], dst_ref=xs.at[from_right + k], send_sem=bs_sem.at[k], recv_sem=br_sem.at[k],
                device_id={"row": p + 1}, device_id_type=MESH)
            bwd.wait_recv()
        last = rows - 1
        g_t[last] = f_t[last] - dot_nt(xs[from_right + k], u_v[last])
        row(last, last - 1, final)

        @pl.when(has_right)
        def _():
            send_right(k).start()

        if not final:
            @pl.loop(0, rows - 1)
            def _(i):
                g_t[i] = f_t[i] - dot_nt(xs[i + 1], u_v[i])

    @pl.loop(0, SWEEPS - 1)
    def _(k):
        sweep(k, False)
    sweep(SWEEPS - 1, True)

    @pl.when(has_right)
    def _():
        send_right(SWEEPS - 1).wait_send()
    for i in (rows - 2, rows - 1):
        pltpu.make_async_copy(out_st.at[i % 2], out_hbm.at[i], out_sem.at[i % 2]).wait()


def solution(mesh):
    chain_len = mesh.shape["row"]
    mat_spec = P(("batch", "row"), None, None)
    vec_spec = P(("batch", "row"), None, "col")

    def device_fn(d_inv, l_blk, u_blk, rhs_blk, x_init):
        rows, size, cols = rhs_blk.shape
        any_spec = pl.BlockSpec(memory_space=pl.ANY)
        mat = pltpu.VMEM((rows, size, size), BF16)
        dma = pltpu.SemaphoreType.DMA
        return pl.pallas_call(
            functools.partial(kernel, chain_len, rows),
            out_shape=jax.ShapeDtypeStruct(rhs_blk.shape, F32),
            in_specs=[any_spec] * 5,
            out_specs=any_spec,
            scratch_shapes=[
                mat, mat, mat,
                pltpu.VMEM((rows, cols, size), F32),
                pltpu.VMEM((rows, cols, size), F32),
                pltpu.VMEM((rows + 2 * SWEEPS, cols, size), BF16),
                pltpu.VMEM((2, size, cols), F32),
                pltpu.VMEM((2, size, cols), F32),
                pltpu.VMEM((8, 128), F32),
                pltpu.VMEM((2, size, cols), F32),
                dma((rows,)), dma((rows,)), dma((rows,)), dma((2,)), dma((2,)), dma((2,)),
                dma((SWEEPS,)), dma((SWEEPS,)), dma((SWEEPS,)), dma((SWEEPS,)),
            ],
            compiler_params=pltpu.CompilerParams(
                collective_id=0, has_side_effects=True, vmem_limit_bytes=67043328),
        )(d_inv, l_blk, u_blk, rhs_blk, x_init)

    return jax.shard_map(device_fn, mesh=mesh, in_specs=(mat_spec, mat_spec, mat_spec, vec_spec, vec_spec),
                         out_specs=vec_spec, check_vma=False)
```

```python
import functools

import jax
import jax.numpy as jnp
from jax import lax
from jax.experimental import pallas as pl
from jax.experimental.pallas import tpu as pltpu
from jax.sharding import PartitionSpec as P

SWEEPS = 4
TILE = 256
MESH = pl.DeviceIdType.MESH
F32, BF16 = jnp.float32, jnp.bfloat16


def dot_nn(x, mat):
    return jnp.dot(x, mat, preferred_element_type=F32)


def dot_nt(x, mat):
    return lax.dot_general(x, mat, (((1,), (1,)), ((), ())), preferred_element_type=F32)


def kernel(chain_len, rows, d_hbm, l_hbm, u_hbm, f_hbm, x_hbm, out_hbm,
           d_v, l_v, u_v, f_v, g_v, xs, x_raw, out_st,
           d_sem, l_sem, u_sem, f_sem, x_sem, out_sem,
           fs_sem, fr_sem, bs_sem, br_sem):
    p = lax.axis_index("row")
    size = d_v.shape[1]
    tiles = size // TILE
    has_left, has_right = p > 0, p < chain_len - 1
    from_left, from_right = rows, rows + SWEEPS

    def mat_copies(i):
        return (pltpu.make_async_copy(u_hbm.at[i], u_v.at[i], u_sem.at[i]),
                pltpu.make_async_copy(l_hbm.at[i], l_v.at[i], l_sem.at[i]),
                pltpu.make_async_copy(d_hbm.at[i], d_v.at[i], d_sem.at[i]))

    def f_copy(i):
        return pltpu.make_async_copy(f_hbm.at[i], f_v.at[i], f_sem.at[i])

    def x_copy(i, slot):
        return pltpu.make_async_copy(x_hbm.at[i], x_raw.at[slot], x_sem.at[slot])

    def send_right(k):
        return pltpu.make_async_remote_copy(
            src_ref=xs.at[rows - 1], dst_ref=xs.at[from_left + k], send_sem=fs_sem.at[k], recv_sem=fr_sem.at[k],
            device_id={"row": p + 1}, device_id_type=MESH)

    def send_left(k):
        return pltpu.make_async_remote_copy(
            src_ref=xs.at[0], dst_ref=xs.at[from_right + k], send_sem=bs_sem.at[k], recv_sem=br_sem.at[k],
            device_id={"row": p - 1}, device_id_type=MESH)

    x_copy(0, 0).start()
    x_copy(1, 1).start()
    f_copy(0).start()
    f_copy(1).start()
    for i in range(2):
        for c in mat_copies(i):
            c.start()

    barrier = pltpu.get_barrier_semaphore()

    @pl.when(has_left)
    def _():
        pl.semaphore_signal(barrier, inc=1, device_id={"row": p - 1}, device_id_type=MESH)

    @pl.when(has_right)
    def _():
        pl.semaphore_signal(barrier, inc=1, device_id={"row": p + 1}, device_id_type=MESH)

    pl.semaphore_wait(barrier, has_left.astype(jnp.int32) + has_right.astype(jnp.int32))

    zero = jnp.zeros(xs.shape[1:], BF16)

    @pl.when(jnp.logical_not(has_left))
    def _():
        for k in range(SWEEPS):
            xs[from_left + k] = zero

    @pl.when(jnp.logical_not(has_right))
    def _():
        for k in range(SWEEPS):
            xs[from_right + k] = zero

    def load_x(i, slot):
        x_copy(i, slot).wait()
        xs[i] = x_raw[slot].astype(BF16)

    def transpose_in_place(ref, i):
        def at(a, b):
            return ref.at[i, a * TILE:(a + 1) * TILE, b * TILE:(b + 1) * TILE]
        for a in range(tiles):
            at(a, a)[...] = at(a, a)[...].T
            for b in range(a + 1, tiles):
                upper, lower = at(a, b)[...].T, at(b, a)[...].T
                at(a, b)[...] = lower
                at(b, a)[...] = upper

    load_x(0, 0)
    x_copy(2, 0).start()

    @pl.when(has_left)
    def _():
        send_left(0).start()

    def load_row(i, last=False):
        slot = lax.rem(i, 2)
        if not last:
            @pl.when(i + 2 < rows)
            def _():
                f_copy(i + 2).start()
                for c in mat_copies(i + 2):
                    c.start()
            load_x(i + 1, 1 - slot)

            @pl.when(i + 3 < rows)
            def _():
                x_copy(i + 3, 1 - slot).start()
        f_copy(i).wait()
        u_c, l_c, d_c = mat_copies(i)
        l_c.wait()
        transpose_in_place(l_v, i)
        d_c.wait()
        transpose_in_place(d_v, i)
        u_c.wait()
        if not last:
            g_v[i] = f_v[i] - dot_nt(xs[i + 1], u_v[i])

    @pl.loop(0, rows - 1)
    def _(i):
        load_row(i)
    load_row(rows - 1, last=True)

    def row(i, left, final):
        t = g_v[i] - dot_nn(xs[left], l_v[i])
        x = dot_nn(t.astype(BF16), d_v[i])
        xs[i] = x.astype(BF16)
        if final:
            st = lax.rem(i, 2)

            @pl.when(i >= 2)
            def _():
                pltpu.make_async_copy(out_st.at[st], out_hbm.at[i - 2], out_sem.at[st]).wait()
            out_st[st] = x
            pltpu.make_async_copy(out_st.at[st], out_hbm.at[i], out_sem.at[st]).start()

    def sweep(k, final):
        @pl.when(has_left)
        def _():
            send_left(k).wait_send()
            fwd = pltpu.make_async_remote_copy(
                src_ref=xs.at[rows - 1], dst_ref=xs.at[from_left + k], send_sem=fs_sem.at[k], recv_sem=fr_sem.at[k],
                device_id={"row": p - 1}, device_id_type=MESH)
            fwd.wait_recv()

        @pl.when(jnp.logical_and(has_right, k > 0))
        def _():
            send_right(k - 1).wait_send()

        row(0, from_left + k, final)
        if not final:
            @pl.when(has_left)
            def _():
                send_left(k + 1).start()

        @pl.loop(1, rows - 1)
        def _(i):
            row(i, i - 1, final)

        @pl.when(has_right)
        def _():
            bwd = pltpu.make_async_remote_copy(
                src_ref=xs.at[0], dst_ref=xs.at[from_right + k], send_sem=bs_sem.at[k], recv_sem=br_sem.at[k],
                device_id={"row": p + 1}, device_id_type=MESH)
            bwd.wait_recv()
        last = rows - 1
        g_v[last] = f_v[last] - dot_nt(xs[from_right + k], u_v[last])
        row(last, last - 1, final)

        @pl.when(has_right)
        def _():
            send_right(k).start()

        if not final:
            @pl.loop(0, rows - 1)
            def _(i):
                g_v[i] = f_v[i] - dot_nt(xs[i + 1], u_v[i])

    @pl.loop(0, SWEEPS - 1)
    def _(k):
        sweep(k, False)
    sweep(SWEEPS - 1, True)

    @pl.when(has_right)
    def _():
        send_right(SWEEPS - 1).wait_send()
    for i in (rows - 2, rows - 1):
        pltpu.make_async_copy(out_st.at[i % 2], out_hbm.at[i], out_sem.at[i % 2]).wait()


def solution(mesh):
    chain_len = mesh.shape["row"]
    mat_spec = P(("batch", "row"), None, None)
    vec_spec = P(("batch", "row"), None, "col")

    def device_fn(d_inv, l_blk, u_blk, rhs_blk, x_init):
        rhs_blk, x_init = jnp.swapaxes(rhs_blk, 1, 2), jnp.swapaxes(x_init, 1, 2)
        rows, cols, size = rhs_blk.shape
        any_spec = pl.BlockSpec(memory_space=pl.ANY)
        mat = pltpu.VMEM((rows, size, size), BF16)
        dma = pltpu.SemaphoreType.DMA
        x_final = pl.pallas_call(
            functools.partial(kernel, chain_len, rows),
            out_shape=jax.ShapeDtypeStruct(rhs_blk.shape, F32),
            in_specs=[any_spec] * 5,
            out_specs=any_spec,
            scratch_shapes=[
                mat, mat, mat,
                pltpu.VMEM((rows, cols, size), F32),
                pltpu.VMEM((rows, cols, size), F32),
                pltpu.VMEM((rows + 2 * SWEEPS, cols, size), BF16),
                pltpu.VMEM((2, cols, size), F32),
                pltpu.VMEM((2, cols, size), F32),
                dma((rows,)), dma((rows,)), dma((rows,)), dma((rows,)), dma((2,)), dma((2,)),
                dma((SWEEPS,)), dma((SWEEPS,)), dma((SWEEPS,)), dma((SWEEPS,)),
            ],
            compiler_params=pltpu.CompilerParams(
                collective_id=0, has_side_effects=True, vmem_limit_bytes=67043328),
        )(d_inv, l_blk, u_blk, rhs_blk, x_init)
        return jnp.swapaxes(x_final, 1, 2)

    return jax.shard_map(device_fn, mesh=mesh, in_specs=(mat_spec, mat_spec, mat_spec, vec_spec, vec_spec),
                         out_specs=vec_spec, check_vma=False)
```

```python
import functools

import jax
import jax.numpy as jnp
from jax import lax
from jax.experimental import pallas as pl
from jax.experimental.pallas import tpu as pltpu
from jax.sharding import PartitionSpec as P

SWEEPS = 4
TILE = 256
MESH = pl.DeviceIdType.MESH
F32, BF16 = jnp.float32, jnp.bfloat16


def dot(x, mat):
    return jnp.dot(x, mat, preferred_element_type=F32)


def kernel(chain_len, rows, d_hbm, l_hbm, u_hbm, f_hbm, x_hbm, out_hbm,
           d_v, l_v, u_v, f_v, g_v, xs, x_raw,
           d_sem, l_sem, u_sem, f_sem, x_sem, out_sem,
           fs_sem, fr_sem, bs_sem, br_sem):
    p = lax.axis_index("row")
    size = d_v.shape[1]
    tiles = size // TILE
    half = size // 2
    halves = (pl.ds(0, half), pl.ds(half, half))
    has_left, has_right = p > 0, p < chain_len - 1
    from_left, from_right = rows, rows + SWEEPS
    last = rows - 1

    def span(t):
        return pl.ds(t * TILE, TILE)

    def mat_copies(i):
        return (pltpu.make_async_copy(l_hbm.at[i], l_v.at[i], l_sem.at[i]),
                pltpu.make_async_copy(d_hbm.at[i], d_v.at[i], d_sem.at[i]),
                pltpu.make_async_copy(u_hbm.at[i], u_v.at[i], u_sem.at[i]))

    def f_copy(i):
        return pltpu.make_async_copy(f_hbm.at[i], f_v.at[i], f_sem.at[i])

    def x_copy(i, slot):
        return pltpu.make_async_copy(x_hbm.at[i], x_raw.at[slot], x_sem.at[slot])

    def out_copy(i):
        return pltpu.make_async_copy(g_v.at[i], out_hbm.at[i], out_sem.at[i])

    def send_right(k, device):
        return pltpu.make_async_remote_copy(
            src_ref=xs.at[last], dst_ref=xs.at[from_left + k], send_sem=fs_sem.at[k], recv_sem=fr_sem.at[k],
            device_id={"row": device}, device_id_type=MESH)

    def send_left(k, device):
        return pltpu.make_async_remote_copy(
            src_ref=xs.at[0], dst_ref=xs.at[from_right + k], send_sem=bs_sem.at[k], recv_sem=br_sem.at[k],
            device_id={"row": device}, device_id_type=MESH)

    x_copy(0, 0).start()
    x_copy(1, 1).start()
    for i in range(2):
        f_copy(i).start()
        for c in mat_copies(i):
            c.start()

    barrier = pltpu.get_barrier_semaphore()

    @pl.when(has_left)
    def _():
        pl.semaphore_signal(barrier, inc=1, device_id={"row": p - 1}, device_id_type=MESH)

    @pl.when(has_right)
    def _():
        pl.semaphore_signal(barrier, inc=1, device_id={"row": p + 1}, device_id_type=MESH)

    pl.semaphore_wait(barrier, has_left.astype(jnp.int32) + has_right.astype(jnp.int32))

    zero = jnp.zeros(xs.shape[1:], BF16)

    @pl.when(jnp.logical_not(has_left))
    def _():
        for k in range(SWEEPS):
            xs[from_left + k] = zero

    @pl.when(jnp.logical_not(has_right))
    def _():
        for k in range(SWEEPS):
            xs[from_right + k] = zero

    def load_x(i, slot):
        x_copy(i, slot).wait()
        xs[i] = x_raw[slot].astype(BF16)

    def transpose_in_place(ref, i):
        def at(a, b):
            return ref.at[i, span(a), span(b)]
        for a in range(tiles):
            at(a, a)[...] = at(a, a)[...].T
            for b in range(a + 1, tiles):
                upper, lower = at(a, b)[...].T, at(b, a)[...].T
                at(a, b)[...] = lower
                at(b, a)[...] = upper

    def ahead(i):
        x = xs[i + 1]
        for h in halves:
            g_v[i, :, h] = f_v[i, :, h] - dot(x, u_v[i, :, h])

    def less_left(base, i, left):
        return [base[i, :, h] - dot(left, l_v[i, :, h]) for h in halves]

    def solve(i, t):
        x = dot(t[0].astype(BF16), d_v[i, halves[0], :]) + dot(t[1].astype(BF16), d_v[i, halves[1], :])
        low = x.astype(BF16)
        xs[i] = low
        g_v[i] = x
        return low

    load_x(0, 0)
    x_copy(2, 0).start()

    @pl.when(has_left)
    def _():
        send_left(0, p - 1).start()

    def load_row(i, end=False):
        slot = lax.rem(i, 2)
        if not end:
            @pl.when(i + 2 < rows)
            def _():
                f_copy(i + 2).start()
                for c in mat_copies(i + 2):
                    c.start()
            load_x(i + 1, 1 - slot)

            @pl.when(i + 3 < rows)
            def _():
                x_copy(i + 3, 1 - slot).start()
        f_copy(i).wait()
        l_c, d_c, u_c = mat_copies(i)
        l_c.wait()
        transpose_in_place(l_v, i)
        d_c.wait()
        transpose_in_place(d_v, i)
        u_c.wait()
        transpose_in_place(u_v, i)
        if not end:
            ahead(i)

    with jax.named_scope("load"):
        @pl.loop(0, rows - 1)
        def _(i):
            load_row(i)
        load_row(last, end=True)

    @pl.loop(0, SWEEPS)
    def _(k):
        final = k == SWEEPS - 1

        def wait_left():
            @pl.when(jnp.logical_and(has_right, k > 0))
            def _():
                send_right(k - 1, p + 1).wait_send()

            @pl.when(has_left)
            def _():
                send_left(k, p - 1).wait_send()
                with jax.named_scope("wait_left"):
                    send_right(k, p - 1).wait_recv()

        def wait_right():
            @pl.when(has_right)
            def _():
                with jax.named_scope("wait_right"):
                    send_left(k, p + 1).wait_recv()

        wait_left()
        left = solve(0, less_left(g_v, 0, xs[from_left + k]))

        @pl.when(jnp.logical_and(has_left, jnp.logical_not(final)))
        def _():
            send_left(k + 1, p - 1).start()

        with jax.named_scope("rows_mid"):
            for i in range(1, last):
                left = solve(i, less_left(g_v, i, left))
            t = less_left(f_v, last, left)

        @pl.when(final)
        def _():
            for i in range(last):
                out_copy(i).start()
        wait_right()
        x = xs[from_right + k]
        solve(last, [t[n] - dot(x, u_v[last, :, h]) for n, h in enumerate(halves)])

        @pl.when(has_right)
        def _():
            send_right(k, p + 1).start()

        with jax.named_scope("ahead"):
            @pl.when(jnp.logical_not(final))
            def _():
                for i in range(last):
                    ahead(i)

    out_copy(last).start()

    @pl.when(has_right)
    def _():
        send_right(SWEEPS - 1, p + 1).wait_send()
    for i in range(rows):
        out_copy(i).wait()


def solution(mesh):
    chain_len = mesh.shape["row"]
    mat_spec = P(("batch", "row"), None, None)
    vec_spec = P(("batch", "row"), None, "col")

    def device_fn(d_inv, l_blk, u_blk, rhs_blk, x_init):
        rhs_blk, x_init = jnp.swapaxes(rhs_blk, 1, 2), jnp.swapaxes(x_init, 1, 2)
        rows, cols, size = rhs_blk.shape
        any_spec = pl.BlockSpec(memory_space=pl.ANY)
        mat = pltpu.VMEM((rows, size, size), BF16)
        vec = pltpu.VMEM((rows, cols, size), F32)
        dma = pltpu.SemaphoreType.DMA
        x_final = pl.pallas_call(
            functools.partial(kernel, chain_len, rows),
            out_shape=jax.ShapeDtypeStruct(rhs_blk.shape, F32),
            in_specs=[any_spec] * 5,
            out_specs=any_spec,
            scratch_shapes=[
                mat, mat, mat, vec, vec,
                pltpu.VMEM((rows + 2 * SWEEPS, cols, size), BF16),
                pltpu.VMEM((2, cols, size), F32),
                dma((rows,)), dma((rows,)), dma((rows,)), dma((rows,)), dma((2,)), dma((rows,)),
                dma((SWEEPS,)), dma((SWEEPS,)), dma((SWEEPS,)), dma((SWEEPS,)),
            ],
            compiler_params=pltpu.CompilerParams(
                collective_id=0, has_side_effects=True, vmem_limit_bytes=67043328),
        )(d_inv, l_blk, u_blk, rhs_blk, x_init)
        return jnp.swapaxes(x_final, 1, 2)

    return jax.shard_map(device_fn, mesh=mesh, in_specs=(mat_spec, mat_spec, mat_spec, vec_spec, vec_spec),
                         out_specs=vec_spec, check_vma=False)
```

```python
import functools

import jax
import jax.numpy as jnp
from jax import lax
from jax.experimental import pallas as pl
from jax.experimental.pallas import tpu as pltpu
from jax.sharding import PartitionSpec as P

SWEEPS = 4
TILE = 256
DEPTH = 3
MESH = pl.DeviceIdType.MESH
F32, BF16 = jnp.float32, jnp.bfloat16


def dot(x, mat):
    return jnp.dot(x, mat, preferred_element_type=F32)


def kernel(chain_len, rows, d_hbm, l_hbm, u_hbm, f_hbm, x_hbm, out_hbm,
           d_v, l_v, u_v, f_v, g_v, xs, x_raw,
           d_sem, l_sem, u_sem, f_sem, x_sem, out_sem,
           fs_sem, fr_sem, bs_sem, br_sem):
    p = lax.axis_index("row")
    size = d_v.shape[1]
    tiles = size // TILE
    has_left, has_right = p > 0, p < chain_len - 1
    from_left, from_right = rows, rows + SWEEPS
    last = rows - 1

    def span(t):
        return pl.ds(t * TILE, TILE)

    def mat_copies(i):
        return (pltpu.make_async_copy(l_hbm.at[i], l_v.at[i], l_sem.at[i]),
                pltpu.make_async_copy(d_hbm.at[i], d_v.at[i], d_sem.at[i]),
                pltpu.make_async_copy(u_hbm.at[i], u_v.at[i], u_sem.at[i]))

    def f_copy(i):
        return pltpu.make_async_copy(f_hbm.at[i], f_v.at[i], f_sem.at[i])

    def x_copy(i, slot):
        return pltpu.make_async_copy(x_hbm.at[i], x_raw.at[slot], x_sem.at[slot])

    def out_copy(i):
        return pltpu.make_async_copy(g_v.at[i], out_hbm.at[i], out_sem.at[i])

    def send_right(k, device):
        return pltpu.make_async_remote_copy(
            src_ref=xs.at[last], dst_ref=xs.at[from_left + k], send_sem=fs_sem.at[k], recv_sem=fr_sem.at[k],
            device_id={"row": device}, device_id_type=MESH)

    def send_left(k, device):
        return pltpu.make_async_remote_copy(
            src_ref=xs.at[0], dst_ref=xs.at[from_right + k], send_sem=bs_sem.at[k], recv_sem=br_sem.at[k],
            device_id={"row": device}, device_id_type=MESH)

    x_copy(0, 0).start()
    x_copy(1, 1).start()
    for i in range(DEPTH):
        f_copy(i).start()
        for c in mat_copies(i):
            c.start()

    barrier = pltpu.get_barrier_semaphore()

    @pl.when(has_left)
    def _():
        pl.semaphore_signal(barrier, inc=1, device_id={"row": p - 1}, device_id_type=MESH)

    @pl.when(has_right)
    def _():
        pl.semaphore_signal(barrier, inc=1, device_id={"row": p + 1}, device_id_type=MESH)

    pl.semaphore_wait(barrier, has_left.astype(jnp.int32) + has_right.astype(jnp.int32))

    zero = jnp.zeros(xs.shape[1:], BF16)

    @pl.when(jnp.logical_not(has_left))
    def _():
        for k in range(SWEEPS):
            xs[from_left + k] = zero

    @pl.when(jnp.logical_not(has_right))
    def _():
        for k in range(SWEEPS):
            xs[from_right + k] = zero

    def load_x(i, slot):
        x_copy(i, slot).wait()
        xs[i] = x_raw[slot].astype(BF16)

    def transpose_in_place(ref, i):
        def at(a, b):
            return ref.at[i, span(a), span(b)]
        for a in range(tiles):
            at(a, a)[...] = at(a, a)[...].T
            for b in range(a + 1, tiles):
                upper, lower = at(a, b)[...].T, at(b, a)[...].T
                at(a, b)[...] = lower
                at(b, a)[...] = upper

    def ahead(i):
        g_v[i] = f_v[i] - dot(xs[i + 1], u_v[i])

    def solve(i, t):
        x = dot(t.astype(BF16), d_v[i])
        low = x.astype(BF16)
        xs[i] = low
        g_v[i] = x
        return low

    def row(i, left):
        return solve(i, g_v[i] - dot(left, l_v[i]))

    def last_left(left):
        g_v[last] = f_v[last] - dot(left, l_v[last])

    load_x(0, 0)
    x_copy(2, 0).start()

    @pl.when(has_left)
    def _():
        send_left(0, p - 1).start()

    def more_loads(i):
        slot = lax.rem(i, 2)

        @pl.when(i + DEPTH < rows)
        def _():
            f_copy(i + DEPTH).start()
            for c in mat_copies(i + DEPTH):
                c.start()
        load_x(i + 1, 1 - slot)

        @pl.when(i + 3 < rows)
        def _():
            x_copy(i + 3, 1 - slot).start()

    mats = (l_v, d_v, u_v)

    with jax.named_scope("load"):
        @pl.when(has_left)
        def _():
            def load_row(i):
                f_copy(i).wait()
                for c, ref in zip(mat_copies(i), mats):
                    c.wait()
                    transpose_in_place(ref, i)

            @pl.loop(0, last)
            def _(i):
                more_loads(i)
                load_row(i)
                ahead(i)
            load_row(last)

        @pl.when(jnp.logical_not(has_left))
        def _():
            def load_row(i, behind):
                f_copy(i).wait()
                for c in mat_copies(i):
                    c.wait()
                transpose_in_place(u_v, i)
                behind()
                transpose_in_place(l_v, i)
                transpose_in_place(d_v, i)

            more_loads(0)
            load_row(0, lambda: None)
            ahead(0)

            @pl.loop(1, last)
            def _(i):
                more_loads(i)
                load_row(i, lambda: row(i - 1, xs[jnp.where(i == 1, from_left, i - 2)]))
                ahead(i)
            load_row(last, lambda: row(last - 1, xs[last - 2]))
            last_left(xs[last - 1])

    @pl.loop(0, SWEEPS)
    def _(k):
        final = k == SWEEPS - 1

        def wait_left():
            @pl.when(jnp.logical_and(has_right, k > 0))
            def _():
                send_right(k - 1, p + 1).wait_send()

            @pl.when(has_left)
            def _():
                send_left(k, p - 1).wait_send()
                with jax.named_scope("wait_left"):
                    send_right(k, p - 1).wait_recv()

        def wait_right():
            @pl.when(has_right)
            def _():
                with jax.named_scope("wait_right"):
                    send_left(k, p + 1).wait_recv()

        @pl.when(jnp.logical_or(has_left, k > 0))
        def _():
            wait_left()
            left = row(0, xs[from_left + k])

            @pl.when(jnp.logical_and(has_left, jnp.logical_not(final)))
            def _():
                send_left(k + 1, p - 1).start()

            with jax.named_scope("rows_mid"):
                for i in range(1, last):
                    left = row(i, left)
                last_left(left)

        @pl.when(final)
        def _():
            for i in range(last):
                out_copy(i).start()
        wait_right()
        solve(last, g_v[last] - dot(xs[from_right + k], u_v[last]))

        @pl.when(has_right)
        def _():
            send_right(k, p + 1).start()

        with jax.named_scope("ahead"):
            @pl.when(jnp.logical_not(final))
            def _():
                for i in range(last):
                    ahead(i)

    out_copy(last).start()

    @pl.when(has_right)
    def _():
        send_right(SWEEPS - 1, p + 1).wait_send()
    for i in range(rows):
        out_copy(i).wait()


def solution(mesh):
    chain_len = mesh.shape["row"]
    mat_spec = P(("batch", "row"), None, None)
    vec_spec = P(("batch", "row"), None, "col")

    def device_fn(d_inv, l_blk, u_blk, rhs_blk, x_init):
        rhs_blk, x_init = jnp.swapaxes(rhs_blk, 1, 2), jnp.swapaxes(x_init, 1, 2)
        rows, cols, size = rhs_blk.shape
        any_spec = pl.BlockSpec(memory_space=pl.ANY)
        mat = pltpu.VMEM((rows, size, size), BF16)
        vec = pltpu.VMEM((rows, cols, size), F32)
        dma = pltpu.SemaphoreType.DMA
        x_final = pl.pallas_call(
            functools.partial(kernel, chain_len, rows),
            out_shape=jax.ShapeDtypeStruct(rhs_blk.shape, F32),
            in_specs=[any_spec] * 5,
            out_specs=any_spec,
            scratch_shapes=[
                mat, mat, mat, vec, vec,
                pltpu.VMEM((rows + 2 * SWEEPS, cols, size), BF16),
                pltpu.VMEM((2, cols, size), F32),
                dma((rows,)), dma((rows,)), dma((rows,)), dma((rows,)), dma((2,)), dma((rows,)),
                dma((SWEEPS,)), dma((SWEEPS,)), dma((SWEEPS,)), dma((SWEEPS,)),
            ],
            compiler_params=pltpu.CompilerParams(
                collective_id=0, has_side_effects=True, vmem_limit_bytes=67043328),
        )(d_inv, l_blk, u_blk, rhs_blk, x_init)
        return jnp.swapaxes(x_final, 1, 2)

    return jax.shard_map(device_fn, mesh=mesh, in_specs=(mat_spec, mat_spec, mat_spec, vec_spec, vec_spec),
                         out_specs=vec_spec, check_vma=False)
```

```python
import functools

import jax
import jax.numpy as jnp
from jax import lax
from jax.experimental import pallas as pl
from jax.experimental.pallas import tpu as pltpu
from jax.sharding import PartitionSpec as P

SWEEPS = 4
TILE = 256
MESH = pl.DeviceIdType.MESH
F32, BF16 = jnp.float32, jnp.bfloat16


def dot(x, mat):
    return jnp.dot(x, mat, preferred_element_type=F32)


def kernel(chain_len, rows, d_hbm, l_hbm, u_hbm, f_hbm, x_hbm, out_hbm,
           d_v, l_v, u_v, f_v, g_v, xs, x_raw,
           d_sem, l_sem, u_sem, f_sem, x_sem, out_sem,
           fs_sem, fr_sem, bs_sem, br_sem):
    p = lax.axis_index("row")
    size = d_v.shape[1]
    tiles = size // TILE
    has_left, has_right = p > 0, p < chain_len - 1
    from_left, from_right = rows, rows + SWEEPS
    last = rows - 1

    def span(t):
        return pl.ds(t * TILE, TILE)

    def mat_copies(i):
        return (pltpu.make_async_copy(l_hbm.at[i], l_v.at[i], l_sem.at[i]),
                pltpu.make_async_copy(d_hbm.at[i], d_v.at[i], d_sem.at[i]),
                pltpu.make_async_copy(u_hbm.at[i], u_v.at[i], u_sem.at[i]))

    def f_copy(i):
        return pltpu.make_async_copy(f_hbm.at[i], f_v.at[i], f_sem.at[i])

    def x_copy(i, slot):
        return pltpu.make_async_copy(x_hbm.at[i], x_raw.at[slot], x_sem.at[slot])

    def out_copy(i):
        return pltpu.make_async_copy(g_v.at[i], out_hbm.at[i], out_sem.at[i])

    def send_right(k, device):
        return pltpu.make_async_remote_copy(
            src_ref=xs.at[last], dst_ref=xs.at[from_left + k], send_sem=fs_sem.at[k], recv_sem=fr_sem.at[k],
            device_id={"row": device}, device_id_type=MESH)

    def send_left(k, device):
        return pltpu.make_async_remote_copy(
            src_ref=xs.at[0], dst_ref=xs.at[from_right + k], send_sem=bs_sem.at[k], recv_sem=br_sem.at[k],
            device_id={"row": device}, device_id_type=MESH)

    def load_x(i, slot):
        x_copy(i, slot).wait()
        xs[i] = x_raw[slot].astype(BF16)

    def start_row(i):
        f_copy(i).start()
        for c in mat_copies(i):
            c.start()

    @pl.when(has_left)
    def _():
        x_copy(0, 0).start()
    x_copy(1, 1).start()
    start_row(0)

    barrier = pltpu.get_barrier_semaphore()

    @pl.when(has_left)
    def _():
        pl.semaphore_signal(barrier, inc=1, device_id={"row": p - 1}, device_id_type=MESH)

    @pl.when(has_right)
    def _():
        pl.semaphore_signal(barrier, inc=1, device_id={"row": p + 1}, device_id_type=MESH)

    pl.semaphore_wait(barrier, has_left.astype(jnp.int32) + has_right.astype(jnp.int32))

    @pl.when(has_left)
    def _():
        load_x(0, 0)
        send_left(0, p - 1).start()
    start_row(1)
    x_copy(2, 0).start()

    zero = jnp.zeros(xs.shape[1:], BF16)

    @pl.when(jnp.logical_not(has_left))
    def _():
        for k in range(SWEEPS):
            xs[from_left + k] = zero

    @pl.when(jnp.logical_not(has_right))
    def _():
        for k in range(SWEEPS):
            xs[from_right + k] = zero

    def transpose_in_place(ref, i):
        def at(a, b):
            return ref.at[i, span(a), span(b)]
        for a in range(tiles):
            at(a, a)[...] = at(a, a)[...].T
            for b in range(a + 1, tiles):
                upper, lower = at(a, b)[...].T, at(b, a)[...].T
                at(a, b)[...] = lower
                at(b, a)[...] = upper

    def ahead(i):
        g_v[i] = f_v[i] - dot(xs[i + 1], u_v[i])

    def solve(i, t):
        x = dot(t.astype(BF16), d_v[i])
        low = x.astype(BF16)
        xs[i] = low
        g_v[i] = x
        return low

    def row(i, left):
        return solve(i, g_v[i] - dot(left, l_v[i]))

    def load_row(i, behind=lambda: None, end=False, skip_l=False):
        slot = lax.rem(i, 2)
        f_copy(i).wait()
        for c in mat_copies(i):
            c.wait()
        if not end:
            load_x(i + 1, 1 - slot)

            @pl.when(i + 2 < rows)
            def _():
                start_row(i + 2)

            @pl.when(i + 3 < rows)
            def _():
                x_copy(i + 3, 1 - slot).start()
        transpose_in_place(u_v, i)
        behind()
        if not end:
            ahead(i)
        if not skip_l:
            transpose_in_place(l_v, i)
        transpose_in_place(d_v, i)

    with jax.named_scope("load"):
        @pl.when(has_left)
        def _():
            @pl.loop(0, last)
            def _(i):
                load_row(i)
            load_row(last, end=True)

        @pl.when(jnp.logical_not(has_left))
        def _():
            load_row(0, skip_l=True)
            load_row(1, lambda: solve(0, g_v[0]))

            @pl.loop(2, last)
            def _(i):
                load_row(i, lambda: row(i - 1, xs[i - 2]))
            load_row(last, lambda: row(last - 1, xs[last - 2]), end=True)

    def last_right(k):
        @pl.when(has_right)
        def _():
            with jax.named_scope("wait_right"):
                send_left(k, p + 1).wait_recv()
        return dot(xs[from_right + k], u_v[last])

    near = jnp.logical_or(lax.rem(p, 2) == 0, jnp.logical_not(has_right))

    with jax.named_scope("last_early"):
        g_v[last] = f_v[last] - last_right(0)

    @pl.when(jnp.logical_not(has_left))
    def _():
        row(last, xs[last - 1])

    @pl.loop(0, SWEEPS)
    def _(k):
        final = k == SWEEPS - 1

        def wait_left():
            @pl.when(jnp.logical_and(has_right, k > 0))
            def _():
                send_right(k - 1, p + 1).wait_send()

            @pl.when(has_left)
            def _():
                send_left(k, p - 1).wait_send()
                with jax.named_scope("wait_left"):
                    send_right(k, p - 1).wait_recv()

        @pl.when(jnp.logical_or(has_left, k > 0))
        def _():
            wait_left()
            left = row(0, xs[from_left + k])

            @pl.when(jnp.logical_and(has_left, jnp.logical_not(final)))
            def _():
                send_left(k + 1, p - 1).start()

            early = jnp.logical_or(near, k == 0)

            @pl.when(early)
            def _():
                with jax.named_scope("rows_early"):
                    old = left
                    for i in range(1, rows):
                        old = row(i, old)

            @pl.when(jnp.logical_not(early))
            def _():
                with jax.named_scope("rows_late"):
                    old = left
                    for i in range(1, last):
                        old = row(i, old)
                    g_v[last] = f_v[last] - dot(old, l_v[last])
                solve(last, g_v[last] - last_right(k))

        @pl.when(has_right)
        def _():
            send_right(k, p + 1).start()

        @pl.when(final)
        def _():
            for i in range(rows):
                out_copy(i).start()

        with jax.named_scope("ahead"):
            @pl.when(jnp.logical_not(final))
            def _():
                for i in range(last):
                    ahead(i)

        @pl.when(jnp.logical_and(near, jnp.logical_not(final)))
        def _():
            with jax.named_scope("last_early"):
                g_v[last] = f_v[last] - last_right(k + 1)


    @pl.when(has_right)
    def _():
        send_right(SWEEPS - 1, p + 1).wait_send()
    for i in range(rows):
        out_copy(i).wait()


def solution(mesh):
    chain_len = mesh.shape["row"]
    mat_spec = P(("batch", "row"), None, None)
    vec_spec = P(("batch", "row"), None, "col")

    def device_fn(d_inv, l_blk, u_blk, rhs_blk, x_init):
        rhs_blk, x_init = jnp.swapaxes(rhs_blk, 1, 2), jnp.swapaxes(x_init, 1, 2)
        rows, cols, size = rhs_blk.shape
        any_spec = pl.BlockSpec(memory_space=pl.ANY)
        mat = pltpu.VMEM((rows, size, size), BF16)
        vec = pltpu.VMEM((rows, cols, size), F32)
        dma = pltpu.SemaphoreType.DMA
        x_final = pl.pallas_call(
            functools.partial(kernel, chain_len, rows),
            out_shape=jax.ShapeDtypeStruct(rhs_blk.shape, F32),
            in_specs=[any_spec] * 5,
            out_specs=any_spec,
            scratch_shapes=[
                mat, mat, mat, vec, vec,
                pltpu.VMEM((rows + 2 * SWEEPS, cols, size), BF16),
                pltpu.VMEM((2, cols, size), F32),
                dma((rows,)), dma((rows,)), dma((rows,)), dma((rows,)), dma((2,)), dma((rows,)),
                dma((SWEEPS,)), dma((SWEEPS,)), dma((SWEEPS,)), dma((SWEEPS,)),
            ],
            compiler_params=pltpu.CompilerParams(
                collective_id=0, has_side_effects=True, vmem_limit_bytes=67043328),
        )(d_inv, l_blk, u_blk, rhs_blk, x_init)
        return jnp.swapaxes(x_final, 1, 2)

    return jax.shard_map(device_fn, mesh=mesh, in_specs=(mat_spec, mat_spec, mat_spec, vec_spec, vec_spec),
                         out_specs=vec_spec, check_vma=False)
```

```python
import functools

import jax
import jax.numpy as jnp
from jax import lax
from jax.experimental import pallas as pl
from jax.experimental.pallas import tpu as pltpu
from jax.sharding import PartitionSpec as P

SWEEPS = 4
TILE = 256
MESH = pl.DeviceIdType.MESH
F32, BF16 = jnp.float32, jnp.bfloat16


def dot(x, mat):
    return jnp.dot(x, mat, preferred_element_type=F32)


def kernel(chain_len, rows, d_hbm, l_hbm, u_hbm, f_hbm, x_hbm, out_hbm,
           d_v, l_v, u_v, f_v, g_v, xs, x_raw,
           d_sem, l_sem, u_sem, f_sem, x_sem, out_sem,
           fs_sem, fr_sem, bs_sem, br_sem):
    p = lax.axis_index("row")
    size = d_v.shape[1]
    tiles = size // TILE
    has_left, has_right = p > 0, p < chain_len - 1
    from_left, from_right = rows, rows + SWEEPS
    last = rows - 1

    def span(t):
        return pl.ds(t * TILE, TILE)

    def l_copy(i):
        return pltpu.make_async_copy(l_hbm.at[i], l_v.at[i], l_sem.at[i])

    def d_copy(i):
        return pltpu.make_async_copy(d_hbm.at[i], d_v.at[i], d_sem.at[i])

    def u_copy(i):
        return pltpu.make_async_copy(u_hbm.at[i], u_v.at[i], u_sem.at[i])

    def f_copy(i):
        return pltpu.make_async_copy(f_hbm.at[i], f_v.at[i], f_sem.at[i])

    def x_copy(i, slot):
        return pltpu.make_async_copy(x_hbm.at[i], x_raw.at[slot], x_sem.at[slot])

    def out_copy(i):
        return pltpu.make_async_copy(g_v.at[i], out_hbm.at[i], out_sem.at[i])

    def send_right(k, device):
        return pltpu.make_async_remote_copy(
            src_ref=xs.at[last], dst_ref=xs.at[from_left + k], send_sem=fs_sem.at[k], recv_sem=fr_sem.at[k],
            device_id={"row": device}, device_id_type=MESH)

    def send_left(k, device):
        return pltpu.make_async_remote_copy(
            src_ref=xs.at[0], dst_ref=xs.at[from_right + k], send_sem=bs_sem.at[k], recv_sem=br_sem.at[k],
            device_id={"row": device}, device_id_type=MESH)

    def load_x(i, slot):
        x_copy(i, slot).wait()
        xs[i] = x_raw[slot].astype(BF16)

    def start_row(i):
        f_copy(i).start()
        for c in (u_copy(i), l_copy(i), d_copy(i)):
            c.start()

    @pl.when(has_left)
    def _():
        x_copy(0, 0).start()
    x_copy(1, 1).start()
    f_copy(0).start()
    u_copy(0).start()
    d_copy(0).start()

    @pl.when(has_left)
    def _():
        l_copy(0).start()

    barrier = pltpu.get_barrier_semaphore()

    @pl.when(has_left)
    def _():
        pl.semaphore_signal(barrier, inc=1, device_id={"row": p - 1}, device_id_type=MESH)

    @pl.when(has_right)
    def _():
        pl.semaphore_signal(barrier, inc=1, device_id={"row": p + 1}, device_id_type=MESH)

    pl.semaphore_wait(barrier, has_left.astype(jnp.int32) + has_right.astype(jnp.int32))

    @pl.when(has_left)
    def _():
        load_x(0, 0)
        send_left(0, p - 1).start()
        d_copy(1).start()
    f_copy(1).start()
    u_copy(1).start()
    l_copy(1).start()
    x_copy(2, 0).start()

    zero = jnp.zeros(xs.shape[1:], BF16)

    @pl.when(jnp.logical_not(has_left))
    def _():
        for k in range(SWEEPS):
            xs[from_left + k] = zero

    @pl.when(jnp.logical_not(has_right))
    def _():
        for k in range(SWEEPS):
            xs[from_right + k] = zero

    def transpose_in_place(ref, i):
        def at(a, b):
            return ref.at[i, span(a), span(b)]
        for a in range(tiles):
            at(a, a)[...] = at(a, a)[...].T
            for b in range(a + 1, tiles):
                upper, lower = at(a, b)[...].T, at(b, a)[...].T
                at(a, b)[...] = lower
                at(b, a)[...] = upper

    def ahead(i):
        g_v[i] = f_v[i] - dot(xs[i + 1], u_v[i])

    def solve(i, t):
        x = dot(t.astype(BF16), d_v[i])
        low = x.astype(BF16)
        xs[i] = low
        g_v[i] = x
        return low

    def row(i, left):
        return solve(i, g_v[i] - dot(left, l_v[i]))

    def last_right(k):
        @pl.when(has_right)
        def _():
            with jax.named_scope("wait_right"):
                send_left(k, p + 1).wait_recv()
        return dot(xs[from_right + k], u_v[last])

    def load_row(i, end=False):
        slot = lax.rem(i, 2)
        for c in (f_copy(i), u_copy(i), l_copy(i), d_copy(i)):
            c.wait()
        if not end:
            load_x(i + 1, 1 - slot)

            @pl.when(i + 2 < rows)
            def _():
                start_row(i + 2)

            @pl.when(i + 3 < rows)
            def _():
                x_copy(i + 3, 1 - slot).start()
        transpose_in_place(u_v, i)
        if not end:
            ahead(i)
        transpose_in_place(l_v, i)
        transpose_in_place(d_v, i)

    def load_block(copies, ref, i, starts=(), behind=lambda: None):
        for c in copies:
            c.wait()
        for c in starts:
            c.start()
        transpose_in_place(ref, i)
        behind()

    with jax.named_scope("load"):
        @pl.when(has_left)
        def _():
            @pl.loop(0, last)
            def _(i):
                load_row(i)
            load_row(last, end=True)

        @pl.when(jnp.logical_not(has_left))
        def _():
            def before(i):
                @pl.when(i == 1)
                def _():
                    load_block((f_copy(i), u_copy(i)), u_v, i, behind=lambda: solve(0, g_v[0]))

                @pl.when(i > 1)
                def _():
                    load_block((f_copy(i), u_copy(i)), u_v, i, behind=lambda: row(i - 1, xs[i - 2]))

            load_x(1, 1)
            load_block((f_copy(0), u_copy(0)), u_v, 0, (d_copy(1), f_copy(2), x_copy(3, 1)), lambda: ahead(0))
            load_block((d_copy(0),), d_v, 0, (u_copy(2),))

            @pl.loop(1, last)
            def _(i):
                slot = lax.rem(i, 2)
                load_x(i + 1, 1 - slot)
                l_copy(i + 1).start()

                @pl.when(i + 2 < rows)
                def _():
                    f_copy(i + 2).start()

                @pl.when(i + 3 < rows)
                def _():
                    x_copy(i + 3, 1 - slot).start()
                before(i)
                load_block((l_copy(i),), l_v, i, (d_copy(i + 1),), lambda: ahead(i))

                @pl.when(i + 2 < rows)
                def _():
                    u_copy(i + 2).start()
                load_block((d_copy(i),), d_v, i)
            l_copy(0).start()
            load_block((f_copy(last), u_copy(last)), u_v, last, behind=lambda: row(last - 1, xs[last - 2]))

            def last_ahead():
                g_v[last] = f_v[last] - dot(xs[from_right], u_v[last])

            def last_left():
                g_v[last] = g_v[last] - dot(xs[last - 1], l_v[last])
            send_left(0, p + 1).wait_recv()
            load_block((l_copy(last),), l_v, last, behind=last_ahead)
            load_block((d_copy(last),), d_v, last, behind=last_left)
            solve(last, g_v[last])

    near = jnp.logical_or(lax.rem(p, 2) == 0, jnp.logical_not(has_right))

    @pl.when(has_left)
    def _():
        with jax.named_scope("last_early"):
            g_v[last] = f_v[last] - last_right(0)

    @pl.loop(0, SWEEPS)
    def _(k):
        final = k == SWEEPS - 1

        def wait_left():
            @pl.when(jnp.logical_and(has_right, k > 0))
            def _():
                send_right(k - 1, p + 1).wait_send()

            @pl.when(has_left)
            def _():
                send_left(k, p - 1).wait_send()
                with jax.named_scope("wait_left"):
                    send_right(k, p - 1).wait_recv()

        @pl.when(jnp.logical_or(has_left, k > 0))
        def _():
            wait_left()
            left = row(0, xs[from_left + k])

            @pl.when(jnp.logical_and(has_left, jnp.logical_not(final)))
            def _():
                send_left(k + 1, p - 1).start()

            early = jnp.logical_or(near, k == 0)

            @pl.when(jnp.logical_and(near, final))
            def _():
                with jax.named_scope("rows_final"):
                    old = left
                    for i in range(1, rows):
                        old = row(i, old)
                        if i in (rows // 2, last - 1):
                            for j in range(0 if i == rows // 2 else rows // 2 + 1, i + 1):
                                out_copy(j).start()

            @pl.when(jnp.logical_and(early, jnp.logical_not(final)))
            def _():
                with jax.named_scope("rows_early"):
                    old = left
                    for i in range(1, rows):
                        old = row(i, old)

            @pl.when(jnp.logical_not(early))
            def _():
                with jax.named_scope("rows_late"):
                    old = left
                    for i in range(1, last):
                        old = row(i, old)
                    g_v[last] = f_v[last] - dot(old, l_v[last])
                solve(last, g_v[last] - last_right(k))

        @pl.when(has_right)
        def _():
            send_right(k, p + 1).start()

        @pl.when(jnp.logical_not(jnp.logical_or(near, jnp.logical_not(final))))
        def _():
            for i in range(last):
                out_copy(i).start()

        @pl.when(final)
        def _():
            out_copy(last).start()

        @pl.when(jnp.logical_not(jnp.logical_or(has_left, k > 0)))
        def _():
            l_copy(0).wait()

        with jax.named_scope("ahead"):
            @pl.when(jnp.logical_not(final))
            def _():
                for i in range(last):
                    ahead(i)

        @pl.when(jnp.logical_and(near, jnp.logical_not(final)))
        def _():
            with jax.named_scope("last_early"):
                g_v[last] = f_v[last] - last_right(k + 1)


    @pl.when(has_right)
    def _():
        send_right(SWEEPS - 1, p + 1).wait_send()
    for i in range(rows):
        out_copy(i).wait()


def solution(mesh):
    chain_len = mesh.shape["row"]
    mat_spec = P(("batch", "row"), None, None)
    vec_spec = P(("batch", "row"), None, "col")

    def device_fn(d_inv, l_blk, u_blk, rhs_blk, x_init):
        rhs_blk, x_init = jnp.swapaxes(rhs_blk, 1, 2), jnp.swapaxes(x_init, 1, 2)
        rows, cols, size = rhs_blk.shape
        any_spec = pl.BlockSpec(memory_space=pl.ANY)
        mat = pltpu.VMEM((rows, size, size), BF16)
        vec = pltpu.VMEM((rows, cols, size), F32)
        dma = pltpu.SemaphoreType.DMA
        x_final = pl.pallas_call(
            functools.partial(kernel, chain_len, rows),
            out_shape=jax.ShapeDtypeStruct(rhs_blk.shape, F32),
            in_specs=[any_spec] * 5,
            out_specs=any_spec,
            scratch_shapes=[
                mat, mat, mat, vec, vec,
                pltpu.VMEM((rows + 2 * SWEEPS, cols, size), BF16),
                pltpu.VMEM((2, cols, size), F32),
                dma((rows,)), dma((rows,)), dma((rows,)), dma((rows,)), dma((2,)), dma((rows,)),
                dma((SWEEPS,)), dma((SWEEPS,)), dma((SWEEPS,)), dma((SWEEPS,)),
            ],
            compiler_params=pltpu.CompilerParams(
                collective_id=0, has_side_effects=True, vmem_limit_bytes=67043328),
        )(d_inv, l_blk, u_blk, rhs_blk, x_init)
        return jnp.swapaxes(x_final, 1, 2)

    return jax.shard_map(device_fn, mesh=mesh, in_specs=(mat_spec, mat_spec, mat_spec, vec_spec, vec_spec),
                         out_specs=vec_spec, check_vma=False)
```

```python
import functools

import jax
import jax.numpy as jnp
from jax import lax
from jax.experimental import pallas as pl
from jax.experimental.pallas import tpu as pltpu
from jax.sharding import PartitionSpec as P

SWEEPS = 4
TILE = 256
CHUNKS = 4
MESH = pl.DeviceIdType.MESH
F32, BF16 = jnp.float32, jnp.bfloat16


def dot(x, mat):
    return jnp.dot(x, mat, preferred_element_type=F32)


def kernel(chain_len, rows, d_hbm, l_hbm, u_hbm, f_hbm, x_hbm, out_hbm,
           d_v, l_v, u_v, f_v, g_v, xs, x_raw,
           d_sem, l_sem, u_sem, f_sem, x_sem, out_sem,
           fs_sem, fr_sem, bs_sem, br_sem):
    p = lax.axis_index("row")
    size = d_v.shape[1]
    tiles = size // TILE
    has_left, has_right = p > 0, p < chain_len - 1
    from_left, from_right = rows, rows + SWEEPS
    last = rows - 1

    def span(t):
        return pl.ds(t * TILE, TILE)

    def l_copy(i):
        return pltpu.make_async_copy(l_hbm.at[i], l_v.at[i], l_sem.at[i])

    def d_copy(i):
        return pltpu.make_async_copy(d_hbm.at[i], d_v.at[i], d_sem.at[i])

    def u_copy(i):
        return pltpu.make_async_copy(u_hbm.at[i], u_v.at[i], u_sem.at[i])

    def f_copy(i):
        return pltpu.make_async_copy(f_hbm.at[i], f_v.at[i], f_sem.at[i])

    def x_copy(i, slot):
        return pltpu.make_async_copy(x_hbm.at[i], x_raw.at[slot], x_sem.at[slot])

    def out_copy(i):
        return pltpu.make_async_copy(g_v.at[i], out_hbm.at[i], out_sem.at[i])

    def chunk(c):
        return pl.ds(c * (size // CHUNKS), size // CHUNKS)

    def send_right(k, device):
        return [pltpu.make_async_remote_copy(
            src_ref=xs.at[last, :, chunk(c)], dst_ref=xs.at[from_left + k, :, chunk(c)],
            send_sem=fs_sem.at[k, c], recv_sem=fr_sem.at[k, c],
            device_id={"row": device}, device_id_type=MESH) for c in range(CHUNKS)]

    def send_left(k, device):
        return [pltpu.make_async_remote_copy(
            src_ref=xs.at[0, :, chunk(c)], dst_ref=xs.at[from_right + k, :, chunk(c)],
            send_sem=bs_sem.at[k, c], recv_sem=br_sem.at[k, c],
            device_id={"row": device}, device_id_type=MESH) for c in range(CHUNKS)]

    def start(copies):
        for c in copies:
            c.start()

    def sent(copies):
        for c in copies:
            c.wait_send()

    def arrived(copies):
        for c in copies:
            c.wait_recv()

    def load_x(i, slot):
        x_copy(i, slot).wait()
        xs[i] = x_raw[slot].astype(BF16)

    def start_row(i):
        f_copy(i).start()
        for c in (u_copy(i), l_copy(i), d_copy(i)):
            c.start()

    @pl.when(has_left)
    def _():
        x_copy(0, 0).start()
    x_copy(1, 1).start()
    f_copy(0).start()
    u_copy(0).start()
    d_copy(0).start()

    @pl.when(has_left)
    def _():
        l_copy(0).start()

    barrier = pltpu.get_barrier_semaphore()

    @pl.when(has_left)
    def _():
        pl.semaphore_signal(barrier, inc=1, device_id={"row": p - 1}, device_id_type=MESH)

    @pl.when(has_right)
    def _():
        pl.semaphore_signal(barrier, inc=1, device_id={"row": p + 1}, device_id_type=MESH)

    pl.semaphore_wait(barrier, has_left.astype(jnp.int32) + has_right.astype(jnp.int32))

    @pl.when(has_left)
    def _():
        load_x(0, 0)
        start(send_left(0, p - 1))
        d_copy(1).start()
    f_copy(1).start()
    u_copy(1).start()
    l_copy(1).start()
    x_copy(2, 0).start()

    zero = jnp.zeros(xs.shape[1:], BF16)

    @pl.when(jnp.logical_not(has_left))
    def _():
        for k in range(SWEEPS):
            xs[from_left + k] = zero

    @pl.when(jnp.logical_not(has_right))
    def _():
        for k in range(SWEEPS):
            xs[from_right + k] = zero

    def transpose_in_place(ref, i):
        def at(a, b):
            return ref.at[i, span(a), span(b)]
        for a in range(tiles):
            at(a, a)[...] = at(a, a)[...].T
            for b in range(a + 1, tiles):
                upper, lower = at(a, b)[...].T, at(b, a)[...].T
                at(a, b)[...] = lower
                at(b, a)[...] = upper

    def ahead(i):
        g_v[i] = f_v[i] - dot(xs[i + 1], u_v[i])

    def solve(i, t):
        x = dot(t.astype(BF16), d_v[i])
        low = x.astype(BF16)
        xs[i] = low
        g_v[i] = x
        return low

    def row(i, left):
        return solve(i, g_v[i] - dot(left, l_v[i]))

    def last_right(k):
        @pl.when(has_right)
        def _():
            with jax.named_scope("wait_right"):
                arrived(send_left(k, p + 1))
        return dot(xs[from_right + k], u_v[last])

    def load_row(i, end=False):
        slot = lax.rem(i, 2)
        for c in (f_copy(i), u_copy(i), l_copy(i), d_copy(i)):
            c.wait()
        if not end:
            load_x(i + 1, 1 - slot)

            @pl.when(i + 2 < rows)
            def _():
                start_row(i + 2)

            @pl.when(i + 3 < rows)
            def _():
                x_copy(i + 3, 1 - slot).start()
        transpose_in_place(u_v, i)
        if not end:
            ahead(i)
        transpose_in_place(l_v, i)
        transpose_in_place(d_v, i)

    def load_block(copies, ref, i, starts=(), behind=lambda: None):
        for c in copies:
            c.wait()
        for c in starts:
            c.start()
        transpose_in_place(ref, i)
        behind()

    with jax.named_scope("load"):
        @pl.when(has_left)
        def _():
            @pl.loop(0, last)
            def _(i):
                load_row(i)
            load_row(last, end=True)

        @pl.when(jnp.logical_not(has_left))
        def _():
            def before(i):
                @pl.when(i == 1)
                def _():
                    load_block((f_copy(i), u_copy(i)), u_v, i, behind=lambda: solve(0, g_v[0]))

                @pl.when(i > 1)
                def _():
                    load_block((f_copy(i), u_copy(i)), u_v, i, behind=lambda: row(i - 1, xs[i - 2]))

            load_x(1, 1)
            load_block((f_copy(0), u_copy(0)), u_v, 0, (d_copy(1), f_copy(2), x_copy(3, 1)), lambda: ahead(0))
            load_block((d_copy(0),), d_v, 0, (u_copy(2),))

            @pl.loop(1, last)
            def _(i):
                slot = lax.rem(i, 2)
                load_x(i + 1, 1 - slot)
                l_copy(i + 1).start()

                @pl.when(i + 2 < rows)
                def _():
                    f_copy(i + 2).start()

                @pl.when(i + 3 < rows)
                def _():
                    x_copy(i + 3, 1 - slot).start()
                before(i)
                load_block((l_copy(i),), l_v, i, (d_copy(i + 1),), lambda: ahead(i))

                @pl.when(i + 2 < rows)
                def _():
                    u_copy(i + 2).start()
                load_block((d_copy(i),), d_v, i)
            l_copy(0).start()
            load_block((f_copy(last), u_copy(last)), u_v, last, behind=lambda: row(last - 1, xs[last - 2]))

            def last_ahead():
                g_v[last] = f_v[last] - dot(xs[from_right], u_v[last])

            def last_left():
                g_v[last] = g_v[last] - dot(xs[last - 1], l_v[last])
            arrived(send_left(0, p + 1))
            load_block((l_copy(last),), l_v, last, behind=last_ahead)
            load_block((d_copy(last),), d_v, last, behind=last_left)
            solve(last, g_v[last])

    far_left = jnp.logical_and(lax.rem(p, 2) == 0, has_left)
    near = jnp.logical_or(lax.rem(p, 2) == 0, jnp.logical_not(has_right))

    @pl.when(has_left)
    def _():
        with jax.named_scope("last_early"):
            g_v[last] = f_v[last] - last_right(0)

    @pl.loop(0, SWEEPS)
    def _(k):
        final = k == SWEEPS - 1

        @pl.when(jnp.logical_or(has_left, k > 0))
        def _():
            @pl.when(jnp.logical_and(has_right, k > 0))
            def _():
                sent(send_right(k - 1, p + 1))

            @pl.when(has_left)
            def _():
                sent(send_left(k, p - 1))

            @pl.when(far_left)
            def _():
                with jax.named_scope("first_far"):
                    t = g_v[0]
                    for c, copy in enumerate(send_right(k, p - 1)):
                        copy.wait_recv()
                        t = t - dot(xs[from_left + k, :, chunk(c)], l_v[0, chunk(c), :])
                        if c < CHUNKS - 1:
                            g_v[0] = t
                            t = g_v[0]
                    solve(0, t)

            @pl.when(jnp.logical_not(far_left))
            def _():
                @pl.when(has_left)
                def _():
                    with jax.named_scope("wait_left"):
                        arrived(send_right(k, p - 1))
                row(0, xs[from_left + k])

            @pl.when(jnp.logical_and(has_left, jnp.logical_not(final)))
            def _():
                start(send_left(k + 1, p - 1))

            early = jnp.logical_or(near, k == 0)

            @pl.when(jnp.logical_and(near, final))
            def _():
                with jax.named_scope("rows_final"):
                    old = xs[0]
                    for i in range(1, rows):
                        old = row(i, old)
                        if i in (rows // 2, last - 1):
                            for j in range(0 if i == rows // 2 else rows // 2 + 1, i + 1):
                                out_copy(j).start()

            @pl.when(jnp.logical_and(early, jnp.logical_not(final)))
            def _():
                with jax.named_scope("rows_early"):
                    old = xs[0]
                    for i in range(1, rows):
                        old = row(i, old)

            @pl.when(jnp.logical_not(early))
            def _():
                with jax.named_scope("rows_late"):
                    old = xs[0]
                    for i in range(1, last):
                        old = row(i, old)
                    g_v[last] = f_v[last] - dot(old, l_v[last])
                solve(last, g_v[last] - last_right(k))

        @pl.when(has_right)
        def _():
            start(send_right(k, p + 1))

        @pl.when(jnp.logical_not(jnp.logical_or(near, jnp.logical_not(final))))
        def _():
            for i in range(last):
                out_copy(i).start()

        @pl.when(final)
        def _():
            out_copy(last).start()

        @pl.when(jnp.logical_not(jnp.logical_or(has_left, k > 0)))
        def _():
            l_copy(0).wait()

        with jax.named_scope("ahead"):
            @pl.when(jnp.logical_not(final))
            def _():
                for i in range(last):
                    ahead(i)

        @pl.when(jnp.logical_and(near, jnp.logical_not(final)))
        def _():
            with jax.named_scope("last_early"):
                g_v[last] = f_v[last] - last_right(k + 1)


    @pl.when(has_right)
    def _():
        sent(send_right(SWEEPS - 1, p + 1))
    for i in range(rows):
        out_copy(i).wait()


def write_out(src, out, buf, in_sem, out_sem):
    n = src.shape[0]
    ins = [pltpu.make_async_copy(src.at[i], buf.at[i], in_sem.at[i]) for i in range(n)]
    outs = [pltpu.make_async_copy(buf.at[i], out.at[i], out_sem.at[i]) for i in range(n)]
    for c in ins:
        c.start()
    for i in range(n):
        ins[i].wait()
        outs[i].start()
    for c in outs:
        c.wait()


def solution(mesh):
    chain_len = mesh.shape["row"]
    mat_spec = P(("batch", "row"), None, None)
    vec_spec = P(("batch", "row"), None, "col")

    def device_fn(d_inv, l_blk, u_blk, rhs_blk, x_init):
        rhs_blk, x_init = jnp.swapaxes(rhs_blk, 1, 2), jnp.swapaxes(x_init, 1, 2)
        rows, cols, size = rhs_blk.shape
        any_spec = pl.BlockSpec(memory_space=pl.ANY)
        mat = pltpu.VMEM((rows, size, size), BF16)
        vec = pltpu.VMEM((rows, cols, size), F32)
        dma = pltpu.SemaphoreType.DMA
        x_final = pl.pallas_call(
            functools.partial(kernel, chain_len, rows),
            out_shape=jax.ShapeDtypeStruct(rhs_blk.shape, F32),
            in_specs=[any_spec] * 5,
            out_specs=any_spec,
            scratch_shapes=[
                mat, mat, mat, vec, vec,
                pltpu.VMEM((rows + 2 * SWEEPS, cols, size), BF16),
                pltpu.VMEM((2, cols, size), F32),
                dma((rows,)), dma((rows,)), dma((rows,)), dma((rows,)), dma((2,)), dma((rows,)),
                *[dma((SWEEPS, CHUNKS))] * 4,
            ],
            compiler_params=pltpu.CompilerParams(
                collective_id=0, has_side_effects=True, vmem_limit_bytes=67043328),
        )(d_inv, l_blk, u_blk, rhs_blk, x_init)
        x_final = pl.pallas_call(
            write_out,
            out_shape=jax.ShapeDtypeStruct(rhs_blk.shape, F32),
            in_specs=[any_spec],
            out_specs=any_spec,
            scratch_shapes=[vec, dma((rows,)), dma((rows,))],
        )(x_final)
        return jnp.swapaxes(x_final, 1, 2)

    return jax.shard_map(device_fn, mesh=mesh, in_specs=(mat_spec, mat_spec, mat_spec, vec_spec, vec_spec),
                         out_specs=vec_spec, check_vma=False)
```

```python
import functools

import jax
import jax.numpy as jnp
from jax import lax
from jax.experimental import pallas as pl
from jax.experimental.pallas import tpu as pltpu
from jax.sharding import PartitionSpec as P

SWEEPS = 4
TILE = 256
CHUNKS = 4
MESH = pl.DeviceIdType.MESH
F32, BF16 = jnp.float32, jnp.bfloat16


def dot(x, mat):
    return jnp.dot(x, mat, preferred_element_type=F32)


def kernel(chain_len, rows, d_hbm, l_hbm, u_hbm, f_hbm, x_hbm, out_hbm,
           d_v, l_v, u_v, f_v, g_v, xs, x_raw,
           d_sem, l_sem, u_sem, f_sem, x_sem, out_sem,
           fs_sem, fr_sem, bs_sem, br_sem):
    p = lax.axis_index("row")
    size = d_v.shape[1]
    tiles = size // TILE
    has_left, has_right = p > 0, p < chain_len - 1
    from_left, from_right = rows, rows + SWEEPS
    last = rows - 1

    def span(t):
        return pl.ds(t * TILE, TILE)

    def l_copy(i):
        return pltpu.make_async_copy(l_hbm.at[i], l_v.at[i], l_sem.at[i])

    def d_copy(i):
        return pltpu.make_async_copy(d_hbm.at[i], d_v.at[i], d_sem.at[i])

    def u_copy(i):
        return pltpu.make_async_copy(u_hbm.at[i], u_v.at[i], u_sem.at[i])

    def f_copy(i):
        return pltpu.make_async_copy(f_hbm.at[i], f_v.at[i], f_sem.at[i])

    def x_copy(i, slot):
        return pltpu.make_async_copy(x_hbm.at[i], x_raw.at[slot], x_sem.at[slot])

    def out_copy(i):
        return pltpu.make_async_copy(g_v.at[i], out_hbm.at[i], out_sem.at[i])

    def chunk(c):
        return pl.ds(c * (size // CHUNKS), size // CHUNKS)

    def send_right(k, device):
        return [pltpu.make_async_remote_copy(
            src_ref=xs.at[last, :, chunk(c)], dst_ref=xs.at[from_left + k, :, chunk(c)],
            send_sem=fs_sem.at[k, c], recv_sem=fr_sem.at[k, c],
            device_id={"row": device}, device_id_type=MESH) for c in range(CHUNKS)]

    def send_left(k, device):
        return [pltpu.make_async_remote_copy(
            src_ref=xs.at[0, :, chunk(c)], dst_ref=xs.at[from_right + k, :, chunk(c)],
            send_sem=bs_sem.at[k, c], recv_sem=br_sem.at[k, c],
            device_id={"row": device}, device_id_type=MESH) for c in range(CHUNKS)]

    def start(copies):
        for c in copies:
            c.start()

    def sent(copies):
        for c in copies:
            c.wait_send()

    def arrived(copies):
        for c in copies:
            c.wait_recv()

    def load_x(i, slot):
        x_copy(i, slot).wait()
        xs[i] = x_raw[slot].astype(BF16)

    def start_row(i):
        f_copy(i).start()
        for c in (u_copy(i), l_copy(i), d_copy(i)):
            c.start()

    @pl.when(has_left)
    def _():
        x_copy(0, 0).start()
    x_copy(1, 1).start()
    f_copy(0).start()
    u_copy(0).start()
    d_copy(0).start()

    @pl.when(has_left)
    def _():
        l_copy(0).start()

    barrier = pltpu.get_barrier_semaphore()

    @pl.when(has_left)
    def _():
        pl.semaphore_signal(barrier, inc=1, device_id={"row": p - 1}, device_id_type=MESH)

    @pl.when(has_right)
    def _():
        pl.semaphore_signal(barrier, inc=1, device_id={"row": p + 1}, device_id_type=MESH)

    pl.semaphore_wait(barrier, has_left.astype(jnp.int32) + has_right.astype(jnp.int32))

    @pl.when(has_left)
    def _():
        load_x(0, 0)
        start(send_left(0, p - 1))
        d_copy(1).start()
    f_copy(1).start()
    u_copy(1).start()
    l_copy(1).start()
    x_copy(2, 0).start()

    zero = jnp.zeros(xs.shape[1:], BF16)

    @pl.when(jnp.logical_not(has_left))
    def _():
        for k in range(SWEEPS):
            xs[from_left + k] = zero

    @pl.when(jnp.logical_not(has_right))
    def _():
        for k in range(SWEEPS):
            xs[from_right + k] = zero

    def transpose_in_place(ref, i):
        def at(a, b):
            return ref.at[i, span(a), span(b)]
        for a in range(tiles):
            at(a, a)[...] = at(a, a)[...].T
            for b in range(a + 1, tiles):
                upper, lower = at(a, b)[...].T, at(b, a)[...].T
                at(a, b)[...] = lower
                at(b, a)[...] = upper

    def ahead(i):
        g_v[i] = f_v[i] - dot(xs[i + 1], u_v[i])

    def solve(i, t):
        x = dot(t.astype(BF16), d_v[i])
        low = x.astype(BF16)
        xs[i] = low
        g_v[i] = x
        return low

    def row(i, left):
        return solve(i, g_v[i] - dot(left, l_v[i]))

    def last_right(k):
        @pl.when(has_right)
        def _():
            with jax.named_scope("wait_right"):
                arrived(send_left(k, p + 1))
        return dot(xs[from_right + k], u_v[last])

    def load_row(i, end=False):
        slot = lax.rem(i, 2)
        for c in (f_copy(i), u_copy(i), l_copy(i), d_copy(i)):
            c.wait()
        if not end:
            load_x(i + 1, 1 - slot)

            @pl.when(i + 2 < rows)
            def _():
                start_row(i + 2)

            @pl.when(i + 3 < rows)
            def _():
                x_copy(i + 3, 1 - slot).start()
        transpose_in_place(u_v, i)
        if not end:
            ahead(i)
        transpose_in_place(l_v, i)
        transpose_in_place(d_v, i)

    def load_block(copies, ref, i, starts=(), behind=lambda: None):
        for c in copies:
            c.wait()
        for c in starts:
            c.start()
        transpose_in_place(ref, i)
        behind()

    with jax.named_scope("load"):
        @pl.when(has_left)
        def _():
            @pl.loop(0, last)
            def _(i):
                load_row(i)
            load_row(last, end=True)

        @pl.when(jnp.logical_not(has_left))
        def _():
            def less_left(i):
                g_v[i] = g_v[i] - dot(xs[i - 1], l_v[i])

            load_x(1, 1)
            load_block((f_copy(0), u_copy(0)), u_v, 0, (d_copy(1), f_copy(2), x_copy(3, 1)), lambda: ahead(0))
            load_block((d_copy(0),), d_v, 0, (u_copy(2),))

            @pl.loop(1, last)
            def _(i):
                slot = lax.rem(i, 2)
                load_x(i + 1, 1 - slot)
                l_copy(i + 1).start()

                @pl.when(i + 2 < rows)
                def _():
                    f_copy(i + 2).start()

                @pl.when(i + 3 < rows)
                def _():
                    x_copy(i + 3, 1 - slot).start()
                load_block((f_copy(i), u_copy(i)), u_v, i, behind=lambda: solve(i - 1, g_v[i - 1]))
                load_block((l_copy(i),), l_v, i, (d_copy(i + 1),), lambda: ahead(i))

                @pl.when(i + 2 < rows)
                def _():
                    u_copy(i + 2).start()
                load_block((d_copy(i),), d_v, i, behind=lambda: less_left(i))
            l_copy(0).start()
            load_block((f_copy(last), u_copy(last)), u_v, last, behind=lambda: solve(last - 1, g_v[last - 1]))

            def last_ahead():
                g_v[last] = f_v[last] - dot(xs[from_right], u_v[last])

            arrived(send_left(0, p + 1))
            load_block((l_copy(last),), l_v, last, behind=last_ahead)
            load_block((d_copy(last),), d_v, last, behind=lambda: less_left(last))
            solve(last, g_v[last])

    far_left = jnp.logical_and(lax.rem(p, 2) == 0, has_left)
    near = jnp.logical_or(lax.rem(p, 2) == 0, jnp.logical_not(has_right))

    @pl.when(has_left)
    def _():
        with jax.named_scope("last_early"):
            g_v[last] = f_v[last] - last_right(0)

    @pl.loop(0, SWEEPS)
    def _(k):
        final = k == SWEEPS - 1

        @pl.when(jnp.logical_or(has_left, k > 0))
        def _():
            @pl.when(jnp.logical_and(has_right, k > 0))
            def _():
                sent(send_right(k - 1, p + 1))

            @pl.when(has_left)
            def _():
                sent(send_left(k, p - 1))

            @pl.when(far_left)
            def _():
                with jax.named_scope("first_far"):
                    t = g_v[0]
                    for c, copy in enumerate(send_right(k, p - 1)):
                        copy.wait_recv()
                        t = t - dot(xs[from_left + k, :, chunk(c)], l_v[0, chunk(c), :])
                        if c < CHUNKS - 1:
                            g_v[0] = t
                            t = g_v[0]
                    solve(0, t)

            @pl.when(jnp.logical_not(far_left))
            def _():
                @pl.when(has_left)
                def _():
                    with jax.named_scope("wait_left"):
                        arrived(send_right(k, p - 1))
                row(0, xs[from_left + k])

            @pl.when(jnp.logical_and(has_left, jnp.logical_not(final)))
            def _():
                start(send_left(k + 1, p - 1))

            early = jnp.logical_or(near, k == 0)

            @pl.when(jnp.logical_and(near, final))
            def _():
                with jax.named_scope("rows_final"):
                    old = xs[0]
                    for i in range(1, rows):
                        old = row(i, old)
                        if i in (rows // 2, last - 1):
                            for j in range(0 if i == rows // 2 else rows // 2 + 1, i + 1):
                                out_copy(j).start()

            @pl.when(jnp.logical_and(early, jnp.logical_not(final)))
            def _():
                with jax.named_scope("rows_early"):
                    old = xs[0]
                    for i in range(1, rows):
                        old = row(i, old)

            @pl.when(jnp.logical_not(early))
            def _():
                with jax.named_scope("rows_late"):
                    old = xs[0]
                    for i in range(1, last):
                        old = row(i, old)
                    g_v[last] = f_v[last] - dot(old, l_v[last])
                solve(last, g_v[last] - last_right(k))

        @pl.when(has_right)
        def _():
            start(send_right(k, p + 1))

        @pl.when(jnp.logical_not(jnp.logical_or(near, jnp.logical_not(final))))
        def _():
            for i in range(last):
                out_copy(i).start()

        @pl.when(final)
        def _():
            out_copy(last).start()

        @pl.when(jnp.logical_not(jnp.logical_or(has_left, k > 0)))
        def _():
            l_copy(0).wait()

        with jax.named_scope("ahead"):
            @pl.when(jnp.logical_not(final))
            def _():
                for i in range(last):
                    ahead(i)

        @pl.when(jnp.logical_and(near, jnp.logical_not(final)))
        def _():
            with jax.named_scope("last_early"):
                g_v[last] = f_v[last] - last_right(k + 1)


    @pl.when(has_right)
    def _():
        sent(send_right(SWEEPS - 1, p + 1))
    for i in range(rows):
        out_copy(i).wait()


def write_out(src, out, buf, in_sem, out_sem):
    n = src.shape[0]
    ins = [pltpu.make_async_copy(src.at[i], buf.at[i], in_sem.at[i]) for i in range(n)]
    outs = [pltpu.make_async_copy(buf.at[i], out.at[i], out_sem.at[i]) for i in range(n)]
    for c in ins:
        c.start()
    for i in range(n):
        ins[i].wait()
        outs[i].start()
    for c in outs:
        c.wait()


def solution(mesh):
    chain_len = mesh.shape["row"]
    mat_spec = P(("batch", "row"), None, None)
    vec_spec = P(("batch", "row"), None, "col")

    def device_fn(d_inv, l_blk, u_blk, rhs_blk, x_init):
        rhs_blk, x_init = jnp.swapaxes(rhs_blk, 1, 2), jnp.swapaxes(x_init, 1, 2)
        rows, cols, size = rhs_blk.shape
        any_spec = pl.BlockSpec(memory_space=pl.ANY)
        mat = pltpu.VMEM((rows, size, size), BF16)
        vec = pltpu.VMEM((rows, cols, size), F32)
        dma = pltpu.SemaphoreType.DMA
        x_final = pl.pallas_call(
            functools.partial(kernel, chain_len, rows),
            out_shape=jax.ShapeDtypeStruct(rhs_blk.shape, F32),
            in_specs=[any_spec] * 5,
            out_specs=any_spec,
            scratch_shapes=[
                mat, mat, mat, vec, vec,
                pltpu.VMEM((rows + 2 * SWEEPS, cols, size), BF16),
                pltpu.VMEM((2, cols, size), F32),
                dma((rows,)), dma((rows,)), dma((rows,)), dma((rows,)), dma((2,)), dma((rows,)),
                *[dma((SWEEPS, CHUNKS))] * 4,
            ],
            compiler_params=pltpu.CompilerParams(
                collective_id=0, has_side_effects=True, vmem_limit_bytes=67043328),
        )(d_inv, l_blk, u_blk, rhs_blk, x_init)
        x_final = pl.pallas_call(
            write_out,
            out_shape=jax.ShapeDtypeStruct(rhs_blk.shape, F32),
            in_specs=[any_spec],
            out_specs=any_spec,
            scratch_shapes=[vec, dma((rows,)), dma((rows,))],
        )(x_final)
        return jnp.swapaxes(x_final, 1, 2)

    return jax.shard_map(device_fn, mesh=mesh, in_specs=(mat_spec, mat_spec, mat_spec, vec_spec, vec_spec),
                         out_specs=vec_spec, check_vma=False)
```
